32 devices in a mesh: seq: 4 (over y, core), tp: 8 (over z, x).
Axes of the slice: x: 2, y: 2, z: 4, core: 2. Of those that a mesh axis runs over, the one named last changes fastest.
Arguments:
- tokens: bfloat16 [4096, 5376], P('seq'), may hold values from -6 to 6
- pre_gain: float32 [5376], replicated, may hold values from 0.5 to 2
- w_query: bfloat16 [5376, 4096], P(None, 'tp'), may hold values from -0.078125 to 0.078125
- key_weight_matrix: bfloat16 [5376, 2048], P(None, 'tp'), may hold values from -0.078125 to 0.078125
- value_weight_matrix: bfloat16 [5376, 2048], P(None, 'tp'), may hold values from -0.078125 to 0.078125
- query_gain: float32 [128], replicated, may hold values from 0.5 to 9
- key_norm_gain: float32 [128], replicated, may hold values from 0.5 to 9
- prior_key_cache: bfloat16 [1024, 2048], P(None, 'tp'), may hold values from -6 to 6
- prior_value_cache: bfloat16 [1024, 2048], P(None, 'tp'), may hold values from -6 to 6
- w_out: bfloat16 [4096, 5376], P('tp'), may hold values from -0.09375 to 0.09375
- post_gain: float32 [5376], replicated, may hold values from 0.5 to 2
Outputs:
- updated: bfloat16 [4096, 5376], P(('seq', 'tp'))
The draws below stay inside these ranges and needn't reach their ends.
All inputs are finite; a program needn't handle non-finite values.
Results may differ from the reference program's by a relative error of at most 0.015.
The reference program's roundings to bfloat16 on the way count: a program that leaves them out, or rounds other values in their place, can miss the bound.
Values may be sent and summed in bfloat16 or wider, within the bound.
A program may use at most 128 MiB of HBM per device.

```python
import math
import jax
import jax.numpy as jnp
from jax import lax

MODEL_WIDTH = 5376
HQ = 32
KEY_VALUE_HEADS = 16
HEAD_DIM = 128
WINDOW_SPAN = 1024
BLOCK_TOKENS = 4096
N_TP = 8


def gain_helper(key):
    low, high = (0.5, 2.0)
    logs = jax.random.uniform(key, (HEAD_DIM,), jnp.float32, math.log(low), math.log(high))
    return jnp.exp(logs).astype(jnp.float32)


def draw_query_gain(key, part):
    return gain_helper(jax.random.fold_in(key, 11))


def draw_key_norm_gain(key, part):
    return gain_helper(jax.random.fold_in(key, 12))


def block_scale(own_key, dims, shards, least, high):
    def one(axis_at, parts):
        steps = jax.random.uniform(jax.random.fold_in(jax.random.fold_in(own_key, 6), axis_at), (parts,), jnp.float32, least / len(shards), high / len(shards))
        return jnp.repeat(jnp.exp(steps), dims[axis_at] // parts).reshape((-1,) + (1,) * (len(dims) - axis_at - 1))

    level = one(*shards[0])
    for cut in shards[1:]:
        level = level * one(*cut)
    return level


def centred(own_key, dims, width, bound, shards=(), held_as=jnp.bfloat16):
    level = block_scale(own_key, dims, shards, -0.22, 0.18) if shards else 1.0
    entries = jax.random.normal(own_key, dims, jnp.float32) * width * level
    return jnp.minimum(jnp.maximum(entries, -bound), bound).astype(held_as)


def setup_inputs(seed: int = 0) -> dict:
    seeds = jax.random.split(jax.random.key(seed), 12)
    tokens = centred(seeds[0], (BLOCK_TOKENS, MODEL_WIDTH), 1.0, 6.0, ((0, 4),))
    pre_gain = jnp.clip(jnp.exp(jax.random.uniform(seeds[1], (MODEL_WIDTH,), jnp.float32, math.log(0.5), math.log(2.0))), 0.5, 2.0)
    w_query = centred(seeds[2], (MODEL_WIDTH, HQ * HEAD_DIM), MODEL_WIDTH ** -0.5, 0.078125, ((1, 8),))
    key_weight_matrix = centred(seeds[3], (MODEL_WIDTH, KEY_VALUE_HEADS * HEAD_DIM), MODEL_WIDTH ** -0.5, 0.078125, ((1, 8),))
    value_weight_matrix = centred(seeds[4], (MODEL_WIDTH, KEY_VALUE_HEADS * HEAD_DIM), MODEL_WIDTH ** -0.5, 0.078125, ((1, 8),))
    query_gain = draw_query_gain(jax.random.fold_in(seeds[11], 71), 0)
    key_norm_gain = draw_key_norm_gain(jax.random.fold_in(seeds[11], 71), 0)
    prior_key_cache = centred(seeds[7], (WINDOW_SPAN, KEY_VALUE_HEADS * HEAD_DIM), 1.0, 6.0, ((1, 8),))
    prior_value_cache = centred(seeds[8], (WINDOW_SPAN, KEY_VALUE_HEADS * HEAD_DIM), 1.0, 6.0, ((1, 8),))
    w_out = centred(seeds[9], (HQ * HEAD_DIM, MODEL_WIDTH), (HQ * HEAD_DIM) ** -0.5, 0.09375, ((0, 8),))
    post_gain = jnp.clip(jnp.exp(jax.random.uniform(seeds[10], (MODEL_WIDTH,), jnp.float32, math.log(0.5), math.log(2.0))), 0.5, 2.0)
    return dict(tokens=tokens, pre_gain=pre_gain, w_query=w_query, key_weight_matrix=key_weight_matrix, value_weight_matrix=value_weight_matrix, query_gain=query_gain, key_norm_gain=key_norm_gain, prior_key_cache=prior_key_cache, prior_value_cache=prior_value_cache, w_out=w_out, post_gain=post_gain)


EPSILON = 1e-06

def root_mean_norm(values, gain):
    mean_square = lax.optimization_barrier(jnp.mean(values * values, axis=-1, keepdims=True))
    return values * lax.rsqrt(mean_square + EPSILON) * gain

def rotary_embed_pairs(values, token_positions):
    half = values.shape[-1] // 2
    exponent = jnp.arange(half, dtype=jnp.float32) * (-2.0 / values.shape[-1])
    frequency = jnp.power(jnp.float32(10000.0), exponent)
    angles = token_positions.astype(jnp.float32)[:, None] * frequency[None, :]
    cosine = jnp.cos(angles)[:, None, :]
    sine = jnp.sin(angles)[:, None, :]
    first = values[..., :half]
    second = values[..., half:]
    return jnp.concatenate([first * cosine - second * sine, second * cosine + first * sine], axis=-1)

def attend_block(query_rows, key_rows, value_rows, scale):
    count = query_rows.shape[0]
    heads = query_rows.shape[1]
    kv_heads = key_rows.shape[1]
    grouped = query_rows.reshape(count, kv_heads, heads // kv_heads, -1).astype(jnp.float32)
    scores = jnp.einsum('bkgd,mkd->kgbm', grouped, key_rows.astype(jnp.float32)) * scale
    row_ids = lax.broadcasted_iota(jnp.int32, (count, key_rows.shape[0]), 0)
    col_ids = lax.broadcasted_iota(jnp.int32, (count, key_rows.shape[0]), 1)
    allowed = (col_ids > row_ids) & (col_ids <= row_ids + WINDOW_SPAN)
    scores = jnp.where(allowed, scores, -jnp.inf)
    highest = lax.optimization_barrier(jnp.max(scores, axis=-1, keepdims=True))
    weights = jnp.exp(scores - highest)
    weights = (weights / lax.optimization_barrier(jnp.sum(weights, axis=-1, keepdims=True))).astype(jnp.bfloat16)
    mixed = jnp.einsum('kgbm,mkd->bkgd', weights.astype(jnp.float32), value_rows.astype(jnp.float32))
    return mixed.astype(jnp.bfloat16).reshape(count, heads, -1)

def reference(tokens, pre_gain, w_query, key_weight_matrix, value_weight_matrix, query_gain, key_norm_gain, prior_key_cache, prior_value_cache, w_out, post_gain):
    inputs = tokens.astype(jnp.float32)
    normed = root_mean_norm(inputs, pre_gain).astype(jnp.bfloat16)
    query_raw = jnp.dot(normed, w_query, preferred_element_type=jnp.float32)
    unnormed_keys = jnp.dot(normed, key_weight_matrix, preferred_element_type=jnp.float32)
    projected_values = jnp.dot(normed, value_weight_matrix, preferred_element_type=jnp.float32)
    token_positions = WINDOW_SPAN + jnp.arange(BLOCK_TOKENS, dtype=jnp.int32)
    queries = rotary_embed_pairs(root_mean_norm(query_raw.reshape(BLOCK_TOKENS, HQ, HEAD_DIM), query_gain), token_positions).astype(jnp.bfloat16)
    block_keys = rotary_embed_pairs(root_mean_norm(unnormed_keys.reshape(BLOCK_TOKENS, KEY_VALUE_HEADS, HEAD_DIM), key_norm_gain), token_positions).astype(jnp.bfloat16)
    block_values = projected_values.astype(jnp.bfloat16).reshape(BLOCK_TOKENS, KEY_VALUE_HEADS, HEAD_DIM)
    joined_keys = jnp.concatenate([prior_key_cache.reshape(WINDOW_SPAN, KEY_VALUE_HEADS, HEAD_DIM), block_keys], axis=0)
    joined_values = jnp.concatenate([prior_value_cache.reshape(WINDOW_SPAN, KEY_VALUE_HEADS, HEAD_DIM), block_values], axis=0)
    size = min(512, BLOCK_TOKENS)
    scale = float(MODEL_WIDTH // HQ) ** (-0.5)

    def one_block(number):
        start = (number * size).astype(jnp.int32)
        query_rows = lax.dynamic_slice_in_dim(queries, start, size, 0)
        key_rows = lax.dynamic_slice_in_dim(joined_keys, start, size + WINDOW_SPAN, 0)
        value_rows = lax.dynamic_slice_in_dim(joined_values, start, size + WINDOW_SPAN, 0)
        return attend_block(query_rows, key_rows, value_rows, scale)
    blocks = lax.map(one_block, jnp.arange(BLOCK_TOKENS // size, dtype=jnp.int32))
    attended = blocks.reshape(BLOCK_TOKENS, HQ * HEAD_DIM)
    group_cols = HQ * HEAD_DIM // N_TP

    def add_group(total, group):
        begin = (group * group_cols).astype(jnp.int32)
        columns = lax.dynamic_slice_in_dim(attended, begin, group_cols, 1)
        rows = lax.dynamic_slice_in_dim(w_out, begin, group_cols, 0)
        term = jnp.dot(columns, rows, preferred_element_type=jnp.float32).astype(jnp.bfloat16)
        term = lax.optimization_barrier(term)
        return (total + term.astype(jnp.float32), None)
    summed, _ = lax.scan(add_group, jnp.zeros((BLOCK_TOKENS, MODEL_WIDTH), jnp.float32), jnp.arange(N_TP, dtype=jnp.int32))
    return (inputs + root_mean_norm(summed, post_gain)).astype(jnp.bfloat16)
```

```python
import functools

import jax
import jax.numpy as jnp
from jax import lax
from jax.experimental import pallas as pl
from jax.experimental.pallas import tpu as pltpu
from jax.sharding import PartitionSpec as P

MODEL_WIDTH = 5376
HQ = 32
WINDOW_SPAN = 1024
EPSILON = 1e-06
LANES = 128
MESH = pl.DeviceIdType.MESH


def rotary_tables(half, token_positions):
    exponent = jnp.arange(half, dtype=jnp.float32) * (-1.0 / half)
    frequency = jnp.power(jnp.float32(10000.0), exponent)
    angles = token_positions.astype(jnp.float32)[:, None] * frequency[None, :]
    return jnp.cos(angles), jnp.sin(angles)


def chunk_count(width):
    for unit in (256, 128):
        if width % unit == 0:
            tiles = width // unit
            return max(n for n in range(1, 8) if tiles % n == 0)
    return 1


def orders(places):
    return [
        sorted(range(places), key=lambda r: (-abs(r - p), r < p)) for p in range(places)
    ]


def flipped(index, bit):
    return index + bit - 2 * bit * ((index // bit) % 2)


def kernel(
    dims,
    tokens_ref, wq_ref, wk_ref, wv_ref, pk_ref, pv_ref, wo_ref,
    pre_ref, post_ref, qg_ref, kg_ref, cos_ref, sin_ref,
    out_ref,
    x_buf, wq_buf, wk_buf, wv_buf, q_buf, k_buf, v_buf, wo_buf, wx_buf, att_buf, got_buf, slots, acc_buf, own_buf,
    tok_sem, w_sem, prior_sem, wo_sem, own_sem, w_send, w_recv, kv_send, kv_recv, sw_send, sw_recv, s_send, s_recv,
):
    seq, tp, head, chunks = dims
    rows, width = tokens_ref.shape
    places = tp // 2
    local = rows // tp
    count = 2 * local
    w_rows = wo_ref.shape[0]
    piece = w_rows // seq
    cols = width // chunks
    bits = []
    bit = seq // 2
    while bit >= 1:
        bits.append(bit)
        bit //= 2
    stages = len(bits)
    s = lax.axis_index("seq")
    t = lax.axis_index("tp")
    side = t % 2
    p = t // 2
    mate = t + 1 - 2 * side
    scale = float(MODEL_WIDTH // HQ) ** (-0.5)
    f32 = jnp.float32

    parts = 4
    part = rows // parts

    def token_load(i):
        return pltpu.make_async_copy(tokens_ref.at[pl.ds(i * part, part)], x_buf.at[pl.ds(i * part, part)], tok_sem.at[i])

    def wo_load(c):
        return pltpu.make_async_copy(wo_ref.at[:, pl.ds(c * cols, cols)], wo_buf.at[c], wo_sem.at[c])

    weight_loads = [
        pltpu.make_async_copy(src, dst, w_sem.at[i])
        for i, (src, dst) in enumerate(((wk_ref, wk_buf), (wv_ref, wv_buf), (wq_ref, wq_buf)))
    ]
    prior_loads = [
        pltpu.make_async_copy(src, dst.at[pl.ds(0, WINDOW_SPAN)], prior_sem.at[i])
        for i, (src, dst) in enumerate(((pk_ref, k_buf), (pv_ref, v_buf)))
    ]
    own_load = pltpu.make_async_copy(tokens_ref.at[pl.ds(pl.multiple_of(t * local, local), local)], own_buf, own_sem)
    for i in range(parts):
        token_load(i).start()
    for load in weight_loads:
        load.start()

    @pl.when(s == 0)
    def _():
        for load in prior_loads:
            load.start()

    barrier = pltpu.get_barrier_semaphore()
    near = [(None, (s, mate))]
    near += [(None, (flipped(s, b), t)) for b in bits]
    near += [((s > 0) & (s % 2 == 0), (s - 1, t)), ((s < seq - 1) & (s % 2 == 1), (s + 1, t))]
    near += [(p > 0, (s, t - 2)), (p < places - 1, (s, t + 2))]
    peers = 0
    for there, device in near:
        if there is None:
            peers = peers + 1
            pl.semaphore_signal(barrier, inc=1, device_id=device, device_id_type=MESH)
        else:
            peers = peers + jnp.where(there, 1, 0)

            @pl.when(there)
            def _(device=device):
                pl.semaphore_signal(barrier, inc=1, device_id=device, device_id_type=MESH)
    pl.semaphore_wait(barrier, peers)

    def w_piece(c, index):
        return wx_buf.at[c, pl.ds(pl.multiple_of(index * piece, piece), piece)]

    def w_first(c):
        return pltpu.make_async_remote_copy(
            src_ref=wo_ref.at[pl.ds(pl.multiple_of(s * piece, piece), piece), pl.ds(c * cols, cols)],
            dst_ref=w_piece(c, s),
            send_sem=w_send.at[c, 0],
            recv_sem=w_recv.at[c, 0],
            device_id=(s, mate),
            device_id_type=MESH,
        )

    def masks(stage):
        held = [0]
        for b in bits[: stage - 1]:
            held = held + [m + b for m in held]
        return held

    def from_mask(m):
        index = s
        for b in bits:
            if m & b:
                index = flipped(index, b)
        return index

    def w_next(c, stage, m):
        b = bits[stage - 1]
        index = from_mask(m)
        return pltpu.make_async_remote_copy(
            src_ref=w_piece(c, index),
            dst_ref=w_piece(c, index),
            send_sem=w_send.at[c, m + b],
            recv_sem=w_recv.at[c, m + b],
            device_id=(flipped(s, b), t),
            device_id_type=MESH,
        )

    def w_arrived(c, m):
        pltpu.make_async_remote_copy(
            src_ref=w_piece(c, from_mask(m)),
            dst_ref=w_piece(c, from_mask(m)),
            send_sem=w_send.at[c, m],
            recv_sem=w_recv.at[c, m],
            device_id=(s, mate),
            device_id_type=MESH,
        ).wait_recv()

    def pump(stage, c):
        if stage == 1:
            w_arrived(c, 0)
        else:
            b = bits[stage - 2]
            for m in masks(stage - 1):
                w_arrived(c, m + b)
        for m in masks(stage):
            w_next(c, stage, m).start()

    def pumps(position):
        for stage in range(1, stages + 1):
            lag = -1 if stage == 1 else stage - 1
            if isinstance(position, int):
                if position == 0 and stage == 1:
                    pump(1, 0)
                c = position - lag
                if 0 <= c < chunks:
                    pump(stage, c)
            else:
                c = position - lag

                @pl.when((c >= 0) & (c < chunks))
                def _(stage=stage, c=c):
                    pump(stage, c)

    def w_ready(c):
        if stages == 0:
            w_arrived(c, 0)
        else:
            b = bits[-1]
            for m in masks(stages):
                w_arrived(c, m + b)
        wo_load(c).wait()

    for c in range(chunks):
        w_first(c).start()
    for c in range(chunks):
        wo_load(c).start()
    own_load.start()

    group = 32
    tiles = width // LANES

    for i in range(parts):
        token_load(i).wait()

        @pl.loop(0, part // group)
        def _(g, i=i):
            at = pl.ds(pl.multiple_of(i * part + g * group, group), group)
            sums = jnp.zeros((group, LANES), f32)
            for j in range(tiles):
                v = x_buf[at, j * LANES : (j + 1) * LANES].astype(f32)
                sums = sums + v * v
            factor = lax.rsqrt(jnp.sum(sums, axis=-1, keepdims=True) * (1.0 / width) + EPSILON)
            for j in range(tiles):
                v = x_buf[at, j * LANES : (j + 1) * LANES].astype(f32)
                gain = pre_ref[:, j * LANES : (j + 1) * LANES]
                x_buf[at, j * LANES : (j + 1) * LANES] = (v * factor * gain).astype(jnp.bfloat16)

    pumps(0)

    row_tile = min(512, rows)

    def project(w_buf, first, size, dst, dst_row, gain_ref):
        @pl.loop(0, rows // row_tile)
        def _(i):
            at = pl.ds(pl.multiple_of(i * row_tile, row_tile), row_tile)
            to = pl.ds(pl.multiple_of(dst_row + i * row_tile, row_tile), row_tile)
            raw = jnp.dot(x_buf[at, :], w_buf[:, first : first + size], preferred_element_type=f32)
            if gain_ref is None:
                dst[to, first : first + size] = raw.astype(jnp.bfloat16)
                return
            cosine = cos_ref[at, :]
            sine = sin_ref[at, :]
            for h in range(size // head):
                u = raw[:, h * head : (h + 1) * head]
                mean_square = jnp.mean(u * u, axis=-1, keepdims=True)
                u = u * lax.rsqrt(mean_square + EPSILON) * gain_ref[...]
                u = u * cosine + pltpu.roll(u, head // 2, 1) * sine
                dst[to, first + h * head : first + (h + 1) * head] = u.astype(jnp.bfloat16)

    def kv_copy(i):
        buf = (k_buf, v_buf)[i]
        return pltpu.make_async_remote_copy(
            src_ref=buf.at[pl.ds(rows, WINDOW_SPAN)],
            dst_ref=buf.at[pl.ds(0, WINDOW_SPAN)],
            send_sem=kv_send.at[i],
            recv_sem=kv_recv.at[i],
            device_id=(s + 1, t),
            device_id_type=MESH,
        )

    q_cols = wq_ref.shape[1]
    kv_cols = wk_ref.shape[1]
    weight_loads[0].wait()
    project(wk_buf, 0, kv_cols, k_buf, WINDOW_SPAN, kg_ref)

    @pl.when(s < seq - 1)
    def _():
        kv_copy(0).start()

    pumps(1)
    weight_loads[1].wait()
    project(wv_buf, 0, kv_cols, v_buf, WINDOW_SPAN, None)

    @pl.when(s < seq - 1)
    def _():
        kv_copy(1).start()

    pumps(2)
    weight_loads[2].wait()
    tile = min(256, q_cols)
    position = 3
    for j in range(q_cols // tile):
        project(wq_buf, j * tile, tile, q_buf, 0, qg_ref)
        pumps(position)
        position += 1

    @pl.when(s == 0)
    def _():
        for load in prior_loads:
            load.wait()

    @pl.when(s > 0)
    def _():
        for i in range(2):
            kv_copy(i).wait_recv()

    table = orders(places)

    def row_block(k):
        r = 0
        for at in range(places):
            for kk in range(places):
                r = r + jnp.where((p == at) & (k == kk), table[at][kk], 0)
        return r

    span = count + WINDOW_SPAN
    group_heads = q_cols // kv_cols

    def attend(k):
        r = row_block(k)
        first = pl.multiple_of(r * count, count)
        row_ids = lax.broadcasted_iota(jnp.int32, (count, span), 0)
        col_ids = lax.broadcasted_iota(jnp.int32, (count, span), 1)
        allowed = (col_ids > row_ids) & (col_ids <= row_ids + WINDOW_SPAN)
        for kv in range(kv_cols // head):
            keys = k_buf[pl.ds(first, span), kv * head : (kv + 1) * head]
            values = v_buf[pl.ds(first, span), kv * head : (kv + 1) * head]
            for g in range(group_heads):
                at = slice((kv * group_heads + g) * head, (kv * group_heads + g + 1) * head)
                scores = lax.dot_general(
                    q_buf[pl.ds(first, count), at], keys, (((1,), (1,)), ((), ())), preferred_element_type=f32
                )
                scores = jnp.where(allowed, scores * scale, -jnp.inf)
                highest = jnp.max(scores, axis=-1, keepdims=True)
                weights = jnp.exp(scores - highest)
                total = jnp.sum(weights, axis=-1, keepdims=True)
                mixed = jnp.dot(weights.astype(jnp.bfloat16), values, preferred_element_type=f32)
                mixed = (mixed / total).astype(jnp.bfloat16)
                att_buf[k, 0, :, at] = mixed[:local]
                att_buf[k, 1, :, at] = mixed[local:]

    def swap(k):
        return pltpu.make_async_remote_copy(
            src_ref=att_buf.at[k, 1 - side],
            dst_ref=got_buf.at[k],
            send_sem=sw_send.at[k],
            recv_sem=sw_recv.at[k],
            device_id=(s, mate),
            device_id_type=MESH,
        )

    def product(k, c):
        return jnp.dot(att_buf[k, side], wo_buf[c], preferred_element_type=f32) + jnp.dot(
            got_buf[k], wx_buf[c], preferred_element_type=f32
        )

    def sum_copy(r, slot, c, place):
        return pltpu.make_async_remote_copy(
            src_ref=slots.at[r, c],
            dst_ref=slots.at[slot, c],
            send_sem=s_send.at[r, c],
            recv_sem=s_recv.at[slot, c],
            device_id=(s, 2 * place + side),
            device_id_type=MESH,
        )

    def push(k, c):
        r = row_block(k)
        right = r > p
        inner = jnp.where(right, p, places - 1 - p) > 0
        total = product(k, c)

        @pl.when(inner)
        def _():
            sum_copy(r, r, c, p).wait_recv()

        total = total + jnp.where(inner, slots[r, c].astype(f32), 0.0)
        slots[r, c] = total.astype(jnp.bfloat16)

        @pl.when(right)
        def _():
            sum_copy(r, r, c, p + 1).start()

        @pl.when(jnp.logical_not(right))
        def _():
            sum_copy(r, jnp.where(r == p - 1, places, r), c, p - 1).start()

    early = min(3, chunks)
    base = position

    @pl.loop(0, places)
    def _(k):
        attend(k)
        swap(k).start()
        pumps(base + k)

        @pl.when(k == 1)
        def _():
            for c in range(early):
                w_ready(c)

        @pl.when(k >= 1)
        def _():
            swap(k - 1).wait_recv()

            @pl.loop(0, early)
            def _(c):
                push(k - 1, c)

    for extra in range(base + places, chunks + stages):
        pumps(extra)

    @pl.loop(early, chunks)
    def _(c):
        w_ready(c)

        @pl.loop(0, places - 1)
        def _(k):
            push(k, c)

    if places == 1:
        for c in range(early):
            w_ready(c)
    last = places - 1
    swap(last).wait_recv()
    own_load.wait()

    def finish(c, square):
        total = product(last, c)

        @pl.when(p > 0)
        def _():
            sum_copy(p, p, c, p).wait_recv()

        @pl.when(p < places - 1)
        def _():
            sum_copy(p, places, c, p).wait_recv()

        total = total + jnp.where(p > 0, slots[p, c].astype(f32), 0.0)
        total = total + jnp.where(p < places - 1, slots[places, c].astype(f32), 0.0)
        acc_buf[c] = total
        return square + jnp.sum(total * total, axis=-1, keepdims=True)

    square = lax.fori_loop(0, chunks, finish, jnp.zeros((local, 1), f32))
    factor = lax.rsqrt(square * (1.0 / width) + EPSILON)
    for c in range(chunks):
        at = slice(c * cols, (c + 1) * cols)
        out_ref[:, at] = (own_buf[:, at].astype(f32) + acc_buf[c] * factor * post_ref[:, at]).astype(out_ref.dtype)

    for c in range(chunks):
        w_first(c).wait_send()
    if stages:
        @pl.loop(0, chunks)
        def _(c):
            for stage in range(1, stages + 1):
                for m in masks(stage):
                    w_next(c, stage, m).wait_send()

    @pl.when(s < seq - 1)
    def _():
        for i in range(2):
            kv_copy(i).wait_send()

    @pl.loop(0, places)
    def _(k):
        swap(k).wait_send()

        @pl.when(k < places - 1)
        def _():
            r = row_block(k)

            @pl.loop(0, chunks)
            def _(c):
                sum_copy(r, r, c, p).wait_send()


def sublayer(
    sizes,
    tokens,
    pre_gain,
    w_query,
    key_weight_matrix,
    value_weight_matrix,
    query_gain,
    key_norm_gain,
    prior_key_cache,
    prior_value_cache,
    w_out,
    post_gain,
):
    seq, tp = sizes
    rows, width = tokens.shape
    head = query_gain.shape[0]
    q_cols, kv_cols = w_query.shape[1], key_weight_matrix.shape[1]
    w_rows = w_out.shape[0]
    local = rows // tp
    places = tp // 2
    chunks = chunk_count(width)
    cols = width // chunks
    token_positions = WINDOW_SPAN + lax.axis_index("seq") * rows + jnp.arange(rows, dtype=jnp.int32)
    cosine, sine = rotary_tables(head // 2, token_positions)
    cosine = jnp.concatenate([cosine, cosine], axis=1)
    sine = jnp.concatenate([-sine, sine], axis=1)
    bf16, f32 = jnp.bfloat16, jnp.float32
    dma = pltpu.SemaphoreType.DMA
    anywhere = pl.BlockSpec(memory_space=pl.ANY)
    vmem = pl.BlockSpec(memory_space=pltpu.VMEM)
    return pl.pallas_call(
        functools.partial(kernel, (seq, tp, head, chunks)),
        out_shape=jax.ShapeDtypeStruct((local, width), tokens.dtype),
        in_specs=[anywhere] * 7 + [vmem] * 6,
        out_specs=vmem,
        scratch_shapes=[
            pltpu.VMEM((rows, width), bf16),
            pltpu.VMEM((width, q_cols), bf16),
            pltpu.VMEM((width, kv_cols), bf16),
            pltpu.VMEM((width, kv_cols), bf16),
            pltpu.VMEM((rows, q_cols), bf16),
            pltpu.VMEM((WINDOW_SPAN + rows, kv_cols), bf16),
            pltpu.VMEM((WINDOW_SPAN + rows, kv_cols), bf16),
            pltpu.VMEM((chunks, w_rows, cols), bf16),
            pltpu.VMEM((chunks, w_rows, cols), bf16),
            pltpu.VMEM((places, 2, local, q_cols), bf16),
            pltpu.VMEM((places, local, q_cols), bf16),
            pltpu.VMEM((places + 1, chunks, local, cols), bf16),
            pltpu.VMEM((chunks, local, cols), f32),
            pltpu.VMEM((local, width), bf16),
            dma((4,)),
            dma((3,)),
            dma((2,)),
            dma((chunks,)),
            dma,
            dma((chunks, seq)),
            dma((chunks, seq)),
            dma((2,)),
            dma((2,)),
            dma((places,)),
            dma((places,)),
            dma((places + 1, chunks)),
            dma((places + 1, chunks)),
        ],
        compiler_params=pltpu.CompilerParams(
            collective_id=0, has_side_effects=True, vmem_limit_bytes=63 * 1024 * 1024
        ),
        cost_estimate=pl.CostEstimate(
            flops=2 * rows * width * (q_cols + 2 * kv_cols + 2 * w_rows),
            bytes_accessed=2 * (rows * width + width * (q_cols + 2 * kv_cols) + w_rows * width),
            transcendentals=0,
        ),
    )(
        tokens,
        w_query,
        key_weight_matrix,
        value_weight_matrix,
        prior_key_cache,
        prior_value_cache,
        w_out,
        pre_gain[None, :],
        post_gain[None, :],
        query_gain[None, :],
        key_norm_gain[None, :],
        cosine,
        sine,
    )


def solution(mesh):
    sizes = (mesh.shape["seq"], mesh.shape["tp"])
    return jax.shard_map(
        functools.partial(sublayer, sizes),
        mesh=mesh,
        in_specs=(
            P("seq", None),
            P(),
            P(None, "tp"),
            P(None, "tp"),
            P(None, "tp"),
            P(),
            P(),
            P(None, "tp"),
            P(None, "tp"),
            P("tp", None),
            P(),
        ),
        out_specs=P(("seq", "tp"), None),
        check_vma=False,
    )
```

```python
import functools

import jax
import jax.numpy as jnp
import numpy as np
from jax import lax
from jax.experimental import pallas as pl
from jax.experimental.pallas import tpu as pltpu
from jax.sharding import PartitionSpec as P

MODEL_WIDTH = 5376
HQ = 32
WINDOW_SPAN = 1024
EPSILON = 1e-06
LANES = 128
MESH = pl.DeviceIdType.MESH


FINE = 32


def rotary_tables(half, first, length):
    frequency = 10000.0 ** (-np.arange(half, dtype=np.float64) / half)
    frequency = np.concatenate([frequency, frequency]).astype(np.float32).astype(np.float64)
    coarse = np.arange(first, first + length, FINE)[:, None] * frequency
    fine = np.arange(FINE)[:, None] * frequency
    tables = [np.cos(coarse), np.sin(coarse), np.cos(fine), np.sin(fine)]
    return [table.astype(np.float32) for table in tables]


def chunk_count(width):
    for unit in (256, 128):
        if width % unit == 0:
            tiles = width // unit
            return max(n for n in range(1, 8) if tiles % n == 0)
    return 1


def helped_chunks(chunks, places):
    if places < 4:
        return []
    return list(range(1, chunks, 2))


def orders(places):
    return [
        sorted(range(places), key=lambda r: (-abs(r - p), r < p)) for p in range(places)
    ]


def flipped(index, bit):
    return index + bit - 2 * bit * ((index // bit) % 2)


def kernel(
    dims,
    tokens_ref, wq_ref, wk_ref, wv_ref, pk_ref, pv_ref, wo_ref,
    cc_ref, cs_ref, pre_ref, post_ref, qg_ref, kg_ref, fc_ref, fs_ref,
    out_ref,
    x_buf, wq_buf, wk_buf, wv_buf, q_buf, k_buf, v_buf, wo_buf, wx_buf, att_buf, got_buf, slots, acc_buf, own_buf, we_buf, ea_buf, cc_buf, cs_buf, cos_ref, sin_ref,
    rot_sem, tok_sem, w_sem, prior_sem, wo_sem, own_sem, w_send, w_recv, kv_send, kv_recv, sw_send, sw_recv, s_send, s_recv,
    e_send, e_recv, ea_send, ea_recv,
):
    seq, tp, head, chunks = dims
    rows, width = tokens_ref.shape
    places = tp // 2
    local = rows // tp
    count = 2 * local
    w_rows = wo_ref.shape[0]
    piece = w_rows // seq
    cols = width // chunks
    helped = helped_chunks(chunks, places)
    bits = []
    bit = seq // 2
    while bit >= 1:
        bits.append(bit)
        bit //= 2
    stages = len(bits)
    s = lax.axis_index("seq")
    t = lax.axis_index("tp")
    side = t % 2
    p = t // 2
    mate = t + 1 - 2 * side
    at_end = (p == 0) | (p == places - 1)
    by_end = (p == 1) | (p == places - 2)
    end = jnp.where(p == 1, 0, places - 1)
    scale = float(MODEL_WIDTH // HQ) ** (-0.5)
    f32 = jnp.float32

    parts = 4
    part = rows // parts

    def token_load(i):
        return pltpu.make_async_copy(tokens_ref.at[pl.ds(i * part, part)], x_buf.at[pl.ds(i * part, part)], tok_sem.at[i])

    def wo_load(c):
        return pltpu.make_async_copy(wo_ref.at[:, pl.ds(c * cols, cols)], wo_buf.at[c], wo_sem.at[c])

    weight_loads = [
        pltpu.make_async_copy(src, dst, w_sem.at[i])
        for i, (src, dst) in enumerate(((wk_ref, wk_buf), (wv_ref, wv_buf), (wq_ref, wq_buf)))
    ]
    prior_loads = [
        pltpu.make_async_copy(src, dst.at[pl.ds(0, WINDOW_SPAN)], prior_sem.at[i])
        for i, (src, dst) in enumerate(((pk_ref, k_buf), (pv_ref, v_buf)))
    ]
    own_load = pltpu.make_async_copy(tokens_ref.at[pl.ds(pl.multiple_of(t * local, local), local)], own_buf, own_sem)
    for i in range(parts):
        token_load(i).start()
    weight_loads[0].start()
    coarse_rows = rows // FINE
    table_loads = [
        pltpu.make_async_copy(src.at[pl.ds(pl.multiple_of(s * coarse_rows, 8), coarse_rows)], dst, rot_sem.at[i])
        for i, (src, dst) in enumerate(((cc_ref, cc_buf), (cs_ref, cs_buf)))
    ]
    for load in table_loads:
        load.start()

    @pl.when(s == 0)
    def _():
        for load in prior_loads:
            load.start()

    barrier = pltpu.get_barrier_semaphore()
    near = [(None, (s, mate))]
    near += [(None, (flipped(s, b), t)) for b in bits]
    near += [((s > 0) & (s % 2 == 0), (s - 1, t)), ((s < seq - 1) & (s % 2 == 1), (s + 1, t))]
    near += [(p > 0, (s, t - 2)), (p < places - 1, (s, t + 2))]
    peers = 0
    for there, device in near:
        if there is None:
            peers = peers + 1
            pl.semaphore_signal(barrier, inc=1, device_id=device, device_id_type=MESH)
        else:
            peers = peers + jnp.where(there, 1, 0)

            @pl.when(there)
            def _(device=device):
                pl.semaphore_signal(barrier, inc=1, device_id=device, device_id_type=MESH)
    pl.semaphore_wait(barrier, peers)

    def w_piece(c, index):
        return wx_buf.at[c, pl.ds(pl.multiple_of(index * piece, piece), piece)]

    def w_first(c):
        return pltpu.make_async_remote_copy(
            src_ref=wo_ref.at[pl.ds(pl.multiple_of(s * piece, piece), piece), pl.ds(c * cols, cols)],
            dst_ref=w_piece(c, s),
            send_sem=w_send.at[c, 0],
            recv_sem=w_recv.at[c, 0],
            device_id=(s, mate),
            device_id_type=MESH,
        )

    def masks(stage):
        held = [0]
        for b in bits[: stage - 1]:
            held = held + [m + b for m in held]
        return held

    def from_mask(m):
        index = s
        for b in bits:
            if m & b:
                index = flipped(index, b)
        return index

    def w_next(c, stage, m):
        b = bits[stage - 1]
        index = from_mask(m)
        return pltpu.make_async_remote_copy(
            src_ref=w_piece(c, index),
            dst_ref=w_piece(c, index),
            send_sem=w_send.at[c, m + b],
            recv_sem=w_recv.at[c, m + b],
            device_id=(flipped(s, b), t),
            device_id_type=MESH,
        )

    def w_arrived(c, m):
        pltpu.make_async_remote_copy(
            src_ref=w_piece(c, from_mask(m)),
            dst_ref=w_piece(c, from_mask(m)),
            send_sem=w_send.at[c, m],
            recv_sem=w_recv.at[c, m],
            device_id=(s, mate),
            device_id_type=MESH,
        ).wait_recv()

    def pump(stage, c):
        if stage == 1:
            w_arrived(c, 0)
        else:
            b = bits[stage - 2]
            for m in masks(stage - 1):
                w_arrived(c, m + b)
        for m in masks(stage):
            w_next(c, stage, m).start()

    def w_ready(c):
        if stages == 0:
            w_arrived(c, 0)
        else:
            b = bits[-1]
            for m in masks(stages):
                w_arrived(c, m + b)
        wo_load(c).wait()

    def e_copy(f, half, m, src, index, device):
        return pltpu.make_async_remote_copy(
            src_ref=src,
            dst_ref=we_buf.at[f, half, pl.ds(pl.multiple_of(index * piece, piece), piece)],
            send_sem=e_send.at[f, half, m],
            recv_sem=e_recv.at[f, half, m],
            device_id=device,
            device_id_type=MESH,
        )

    def e_piece(f, half, index):
        return we_buf.at[f, half, pl.ds(pl.multiple_of(index * piece, piece), piece)]

    def e_first(f, m):
        index = from_mask(m)
        src = wo_ref.at[pl.ds(pl.multiple_of(index * piece, piece), piece), pl.ds(helped[f] * cols, cols)]
        return e_copy(f, 0, m, src, index, (s, 2 * jnp.where(p == 0, 1, places - 2) + side))

    def e_mate(f):
        return e_copy(f, 1, 0, e_piece(f, 0, s), s, (s, mate))

    def e_next(f, half, stage, m):
        b = bits[stage - 1]
        index = from_mask(m)
        return e_copy(f, half, m + b, e_piece(f, half, index), index, (flipped(s, b), t))

    def e_arrived(f, half, m):
        index = from_mask(m)
        e_copy(f, half, m, e_piece(f, half, index), index, (s, mate)).wait_recv()

    def e_pump(stage, f):
        @pl.when(by_end)
        def _():
            if stage == 0:
                e_arrived(f, 0, 0)
                e_mate(f).start()
                return
            if stage == 1:
                e_arrived(f, 1, 0)
            else:
                for m in masks(stage - 1):
                    e_arrived(f, 1, m + bits[stage - 2])
            for m in masks(stage):
                e_next(f, 1, stage, m).start()
                if stage == stages:
                    if m:
                        e_arrived(f, 0, m)
                    e_next(f, 0, stage, m).start()

    def e_ready(f):
        @pl.when(by_end)
        def _():
            if stages == 0:
                e_arrived(f, 1, 0)
            else:
                for half in range(2):
                    for m in masks(stages):
                        e_arrived(f, half, m + bits[-1])

    for c in range(chunks):
        w_first(c).start()

    @pl.when(at_end)
    def _():
        for f in range(len(helped)):
            for m in masks(stages):
                e_first(f, m).start()

    for load in table_loads:
        load.wait()
    sign = jnp.where(lax.broadcasted_iota(jnp.int32, (FINE, head), 1) < head // 2, -1.0, 1.0)
    for i in range(coarse_rows):
        far_c, far_s = cc_buf[i : i + 1, :], cs_buf[i : i + 1, :]
        near_c, near_s = fc_ref[...], fs_ref[...]
        cos_ref[i * FINE : (i + 1) * FINE, :] = far_c * near_c - far_s * near_s
        sin_ref[i * FINE : (i + 1) * FINE, :] = (far_s * near_c + far_c * near_s) * sign

    group = 32
    tiles = width // LANES

    for i in range(parts):
        token_load(i).wait()
        if i == parts - 1:
            weight_loads[1].start()
            weight_loads[2].start()

        @pl.loop(0, part // group)
        def _(g, i=i):
            at = pl.ds(pl.multiple_of(i * part + g * group, group), group)
            sums = jnp.zeros((group, LANES), f32)
            for j in range(tiles):
                v = x_buf[at, j * LANES : (j + 1) * LANES].astype(f32)
                sums = sums + v * v
            factor = lax.rsqrt(jnp.sum(sums, axis=-1, keepdims=True) * (1.0 / width) + EPSILON)
            for j in range(tiles):
                v = x_buf[at, j * LANES : (j + 1) * LANES].astype(f32)
                gain = pre_ref[pl.ds(j * LANES, LANES)][None, :]
                x_buf[at, j * LANES : (j + 1) * LANES] = (v * factor * gain).astype(jnp.bfloat16)

    pump(1, 0)

    row_tile = min(512, rows)

    def project(w_buf, first, size, dst, dst_row, gain_ref):
        @pl.loop(0, rows // row_tile)
        def _(i):
            at = pl.ds(pl.multiple_of(i * row_tile, row_tile), row_tile)
            to = pl.ds(pl.multiple_of(dst_row + i * row_tile, row_tile), row_tile)
            raw = jnp.dot(x_buf[at, :], w_buf[:, first : first + size], preferred_element_type=f32)
            if gain_ref is None:
                dst[to, first : first + size] = raw.astype(jnp.bfloat16)
                return
            cosine = cos_ref[at, :]
            sine = sin_ref[at, :]
            for h in range(size // head):
                u = raw[:, h * head : (h + 1) * head]
                mean_square = jnp.mean(u * u, axis=-1, keepdims=True)
                u = u * lax.rsqrt(mean_square + EPSILON) * gain_ref[...][None, :]
                u = u * cosine + pltpu.roll(u, head // 2, 1) * sine
                dst[to, first + h * head : first + (h + 1) * head] = u.astype(jnp.bfloat16)

    def kv_copy(i):
        buf = (k_buf, v_buf)[i]
        return pltpu.make_async_remote_copy(
            src_ref=buf.at[pl.ds(rows, WINDOW_SPAN)],
            dst_ref=buf.at[pl.ds(0, WINDOW_SPAN)],
            send_sem=kv_send.at[i],
            recv_sem=kv_recv.at[i],
            device_id=(s + 1, t),
            device_id_type=MESH,
        )

    q_cols = wq_ref.shape[1]
    kv_cols = wk_ref.shape[1]
    weight_loads[0].wait()
    project(wk_buf, 0, kv_cols, k_buf, WINDOW_SPAN, kg_ref)

    @pl.when(s < seq - 1)
    def _():
        kv_copy(0).start()

    weight_loads[1].wait()
    project(wv_buf, 0, kv_cols, v_buf, WINDOW_SPAN, None)

    @pl.when(s < seq - 1)
    def _():
        kv_copy(1).start()

    weight_loads[2].wait()
    for c in range(chunks):
        wo_load(c).start()
    own_load.start()
    tile = min(256, q_cols)
    for j in range(q_cols // tile):
        project(wq_buf, j * tile, tile, q_buf, 0, qg_ref)
    for c in range(1, min(3, chunks)):
        pump(1, c)
    for stage in range(2, stages + 1):
        pump(stage, 0)

    @pl.when(s == 0)
    def _():
        for load in prior_loads:
            load.wait()

    @pl.when(s > 0)
    def _():
        for i in range(2):
            kv_copy(i).wait_recv()

    table = orders(places)

    def row_block(k):
        r = 0
        for at in range(places):
            for kk in range(places):
                r = r + jnp.where((p == at) & (k == kk), table[at][kk], 0)
        return r

    span = count + WINDOW_SPAN
    group_heads = q_cols // kv_cols

    def attend(k):
        r = row_block(k)
        first = pl.multiple_of(r * count, count)
        row_ids = lax.broadcasted_iota(jnp.int32, (count, span), 0)
        col_ids = lax.broadcasted_iota(jnp.int32, (count, span), 1)
        allowed = (col_ids > row_ids) & (col_ids <= row_ids + WINDOW_SPAN)
        for kv in range(kv_cols // head):
            keys = k_buf[pl.ds(first, span), kv * head : (kv + 1) * head]
            values = v_buf[pl.ds(first, span), kv * head : (kv + 1) * head]
            for g in range(group_heads):
                at = slice((kv * group_heads + g) * head, (kv * group_heads + g + 1) * head)
                scores = lax.dot_general(
                    q_buf[pl.ds(first, count), at], keys, (((1,), (1,)), ((), ())), preferred_element_type=f32
                )
                scores = jnp.where(allowed, scores * scale, -jnp.inf)
                highest = jnp.max(scores, axis=-1, keepdims=True)
                weights = jnp.exp(scores - highest)
                total = jnp.sum(weights, axis=-1, keepdims=True)
                mixed = jnp.dot(weights.astype(jnp.bfloat16), values, preferred_element_type=f32)
                mixed = (mixed / total).astype(jnp.bfloat16)
                att_buf[k, 0, :, at] = mixed[:local]
                att_buf[k, 1, :, at] = mixed[local:]

    def swap(k):
        return pltpu.make_async_remote_copy(
            src_ref=att_buf.at[k, 1 - side],
            dst_ref=got_buf.at[k],
            send_sem=sw_send.at[k],
            recv_sem=sw_recv.at[k],
            device_id=(s, mate),
            device_id_type=MESH,
        )

    def product(k, c):
        return jnp.dot(att_buf[k, side], wo_buf[c], preferred_element_type=f32) + jnp.dot(
            got_buf[k], wx_buf[c], preferred_element_type=f32
        )

    def sum_copy(r, slot, c, place):
        return pltpu.make_async_remote_copy(
            src_ref=slots.at[r, c],
            dst_ref=slots.at[slot, c],
            send_sem=s_send.at[r, c],
            recv_sem=s_recv.at[slot, c],
            device_id=(s, 2 * place + side),
            device_id_type=MESH,
        )

    def send_on(r, c):
        @pl.when(r > p)
        def _():
            sum_copy(r, r, c, p + 1).start()

        @pl.when(r < p)
        def _():
            sum_copy(r, jnp.where(r == p - 1, places, r), c, p - 1).start()

    def add_on(k, r, c):
        inner = jnp.where(r > p, p, places - 1 - p) > 0
        total = product(k, c)

        @pl.when(inner)
        def _():
            sum_copy(r, r, c, p).wait_recv()

        total = total + jnp.where(inner, slots[r, c].astype(f32), 0.0)
        slots[r, c] = total.astype(jnp.bfloat16)

    def push(k, c):
        r = row_block(k)
        add_on(k, r, c)
        send_on(r, c)

    def end_product(r, f):
        return jnp.dot(ea_buf[r, 0], we_buf[f, 0], preferred_element_type=f32) + jnp.dot(
            ea_buf[r, 1], we_buf[f, 1], preferred_element_type=f32
        )

    def push_helped(k, c, f):
        r = row_block(k)
        help_here = by_end & (r != end)

        @pl.when(help_here)
        def _():
            slots[r, c] = (product(k, c) + end_product(r, f)).astype(jnp.bfloat16)

        @pl.when(jnp.logical_not(help_here | at_end))
        def _():
            add_on(k, r, c)

        @pl.when(jnp.logical_not(at_end))
        def _():
            send_on(r, c)

    def end_rows(k, half, r):
        src = got_buf.at[k] if half else att_buf.at[k, side]
        return pltpu.make_async_remote_copy(
            src_ref=src,
            dst_ref=ea_buf.at[r, half],
            send_sem=ea_send.at[k, half],
            recv_sem=ea_recv.at[r, half],
            device_id=(s, 2 * jnp.where(p == 0, 1, places - 2) + side),
            device_id_type=MESH,
        )

    @pl.loop(0, places)
    def _(k):
        attend(k)
        swap(k).start()

        @pl.when(k == 0)
        def _():
            w_ready(0)

        @pl.when((k < 2) & (k + 3 < chunks))
        def _():
            pump(1, k + 3)

        for f in range(min(len(helped), places)):
            @pl.when(k == f)
            def _(f=f):
                e_pump(0, f)

        for f in range(min(len(helped), places - 2)):
            @pl.when(k == f + 2)
            def _(f=f):
                e_pump(1, f)

        @pl.when(k >= 1)
        def _():
            swap(k - 1).wait_recv()
            push(k - 1, 0)

            if helped:
                @pl.when(at_end & (k < places - 1))
                def _():
                    for half in range(2):
                        end_rows(k - 1, half, row_block(k - 1)).start()

    for f in range(places, len(helped)):
        e_pump(0, f)
    waiting = []
    for c in range(3, chunks):
        if c >= 5:
            waiting.append((c, False))
        if c in helped and helped.index(c) >= places - 2:
            waiting.append((c, True))
    for c in range(1, chunks):
        taken = 0
        while waiting and (taken < 2 or waiting[0][0] <= c):
            which, ends = waiting.pop(0)
            if stages == 0:
                continue
            if ends:
                e_pump(1, helped.index(which))
            else:
                pump(1, which)
            taken += 1
        for stage in range(2, stages + 1):
            pump(stage, c)
            if c in helped:
                e_pump(stage, helped.index(c))
        w_ready(c)
        if c not in helped:
            @pl.loop(0, places - 1)
            def _(k, c=c):
                push(k, c)
        else:
            f = helped.index(c)
            e_ready(f)
            if f == 0:
                @pl.when(by_end)
                def _():
                    @pl.loop(0, places)
                    def _(r):
                        @pl.when((r != end) & (r != p))
                        def _():
                            for half in range(2):
                                end_rows(0, half, r).wait_recv()

            @pl.loop(0, places - 1)
            def _(k, c=c, f=f):
                push_helped(k, c, f)
    if helped:
        @pl.when(at_end)
        def _():
            for half in range(2):
                end_rows(places - 2, half, row_block(places - 2)).start()

    last = places - 1
    swap(last).wait_recv()
    own_load.wait()

    def finish(c, square):
        total = product(last, c)
        ahead, behind = p > 0, p < places - 1
        if c in helped:
            ahead, behind = ahead & (p != 1), behind & (p != places - 2)
            acc_buf[c] = total

            @pl.when(by_end)
            def _():
                if c == helped[0]:
                    for half in range(2):
                        end_rows(0, half, p).wait_recv()
                acc_buf[c] += end_product(p, helped.index(c))

            total = acc_buf[c]

        @pl.when(ahead)
        def _():
            sum_copy(p, p, c, p).wait_recv()

        @pl.when(behind)
        def _():
            sum_copy(p, places, c, p).wait_recv()

        total = total + jnp.where(ahead, slots[p, c].astype(f32), 0.0)
        total = total + jnp.where(behind, slots[places, c].astype(f32), 0.0)
        acc_buf[c] = total
        return square + jnp.sum(total * total, axis=-1, keepdims=True)

    square = jnp.zeros((local, 1), f32)
    for c in range(chunks):
        square = finish(c, square)
    factor = lax.rsqrt(square * (1.0 / width) + EPSILON)
    for c in range(chunks):
        at = slice(c * cols, (c + 1) * cols)
        out_ref[:, at] = (own_buf[:, at].astype(f32) + acc_buf[c] * factor * post_ref[pl.ds(c * cols, cols)][None, :]).astype(out_ref.dtype)

    for c in range(chunks):
        w_first(c).wait_send()
    if stages:
        @pl.loop(0, chunks)
        def _(c):
            for stage in range(1, stages + 1):
                for m in masks(stage):
                    w_next(c, stage, m).wait_send()

    @pl.when(s < seq - 1)
    def _():
        for i in range(2):
            kv_copy(i).wait_send()

    @pl.loop(0, places)
    def _(k):
        swap(k).wait_send()

        @pl.when(k < places - 1)
        def _():
            r = row_block(k)

            for c in range(chunks):
                if c in helped:
                    @pl.when(jnp.logical_not(at_end))
                    def _(c=c):
                        sum_copy(r, r, c, p).wait_send()
                else:
                    sum_copy(r, r, c, p).wait_send()

    if helped:
        @pl.when(at_end)
        def _():
            for f in range(len(helped)):
                for m in masks(stages):
                    e_first(f, m).wait_send()

            @pl.loop(0, places - 1)
            def _(k):
                for half in range(2):
                    end_rows(k, half, row_block(k)).wait_send()

        @pl.when(by_end)
        def _():
            for f in range(len(helped)):
                e_mate(f).wait_send()
                for stage in range(1, stages + 1):
                    for m in masks(stage):
                        e_next(f, 1, stage, m).wait_send()
                        if stage == stages:
                            e_next(f, 0, stage, m).wait_send()


def sublayer(
    sizes,
    tokens,
    pre_gain,
    w_query,
    key_weight_matrix,
    value_weight_matrix,
    query_gain,
    key_norm_gain,
    prior_key_cache,
    prior_value_cache,
    w_out,
    post_gain,
):
    seq, tp = sizes
    rows, width = tokens.shape
    head = query_gain.shape[0]
    q_cols, kv_cols = w_query.shape[1], key_weight_matrix.shape[1]
    w_rows = w_out.shape[0]
    local = rows // tp
    places = tp // 2
    chunks = chunk_count(width)
    cols = width // chunks
    helped = len(helped_chunks(chunks, places))
    tables = rotary_tables(head // 2, WINDOW_SPAN, seq * rows)
    bf16, f32 = jnp.bfloat16, jnp.float32
    dma = pltpu.SemaphoreType.DMA
    anywhere = pl.BlockSpec(memory_space=pl.ANY)
    vmem = pl.BlockSpec(memory_space=pltpu.VMEM)
    return pl.pallas_call(
        functools.partial(kernel, (seq, tp, head, chunks)),
        out_shape=jax.ShapeDtypeStruct((local, width), tokens.dtype),
        in_specs=[anywhere] * 9 + [vmem] * 6,
        out_specs=vmem,
        scratch_shapes=[
            pltpu.VMEM((rows, width), bf16),
            pltpu.VMEM((width, q_cols), bf16),
            pltpu.VMEM((width, kv_cols), bf16),
            pltpu.VMEM((width, kv_cols), bf16),
            pltpu.VMEM((rows, q_cols), bf16),
            pltpu.VMEM((WINDOW_SPAN + rows, kv_cols), bf16),
            pltpu.VMEM((WINDOW_SPAN + rows, kv_cols), bf16),
            pltpu.VMEM((chunks, w_rows, cols), bf16),
            pltpu.VMEM((chunks, w_rows, cols), bf16),
            pltpu.VMEM((places, 2, local, q_cols), bf16),
            pltpu.VMEM((places, local, q_cols), bf16),
            pltpu.VMEM((places + 1, chunks, local, cols), bf16),
            pltpu.VMEM((chunks, local, cols), f32),
            pltpu.VMEM((local, width), bf16),
            pltpu.VMEM((max(helped, 1), 2, w_rows, cols), bf16),
            pltpu.VMEM((places, 2, local, q_cols), bf16),
            pltpu.VMEM((rows // FINE, head), f32),
            pltpu.VMEM((rows // FINE, head), f32),
            pltpu.VMEM((rows, head), f32),
            pltpu.VMEM((rows, head), f32),
            dma((2,)),
            dma((4,)),
            dma((3,)),
            dma((2,)),
            dma((chunks,)),
            dma,
            dma((chunks, seq)),
            dma((chunks, seq)),
            dma((2,)),
            dma((2,)),
            dma((places,)),
            dma((places,)),
            dma((places + 1, chunks)),
            dma((places + 1, chunks)),
            dma((max(helped, 1), 2, seq)),
            dma((max(helped, 1), 2, seq)),
            dma((places, 2)),
            dma((places, 2)),
        ],
        compiler_params=pltpu.CompilerParams(
            collective_id=0, has_side_effects=True, vmem_limit_bytes=63 * 1024 * 1024
        ),
        cost_estimate=pl.CostEstimate(
            flops=2 * rows * width * (q_cols + 2 * kv_cols + 2 * w_rows),
            bytes_accessed=2 * (rows * width + width * (q_cols + 2 * kv_cols) + w_rows * width),
            transcendentals=0,
        ),
    )(
        tokens,
        w_query,
        key_weight_matrix,
        value_weight_matrix,
        prior_key_cache,
        prior_value_cache,
        w_out,
        tables[0],
        tables[1],
        pre_gain,
        post_gain,
        query_gain,
        key_norm_gain,
        tables[2],
        tables[3],
    )


def solution(mesh):
    sizes = (mesh.shape["seq"], mesh.shape["tp"])
    return jax.shard_map(
        functools.partial(sublayer, sizes),
        mesh=mesh,
        in_specs=(
            P("seq", None),
            P(),
            P(None, "tp"),
            P(None, "tp"),
            P(None, "tp"),
            P(),
            P(),
            P(None, "tp"),
            P(None, "tp"),
            P("tp", None),
            P(),
        ),
        out_specs=P(("seq", "tp"), None),
        check_vma=False,
    )
```

```python
import functools

import jax
import jax.numpy as jnp
import numpy as np
from jax import lax
from jax.experimental import pallas as pl
from jax.experimental.pallas import tpu as pltpu
from jax.sharding import PartitionSpec as P

MODEL_WIDTH = 5376
HQ = 32
WINDOW_SPAN = 1024
EPSILON = 1e-06
LANES = 128
LOG2E = 1.4426950408889634
MESH = pl.DeviceIdType.MESH


FINE = 32


def rotary_tables(half, first, length):
    frequency = 10000.0 ** (-np.arange(half, dtype=np.float64) / half)
    frequency = np.concatenate([frequency, frequency]).astype(np.float32).astype(np.float64)
    coarse = np.arange(first, first + length, FINE)[:, None] * frequency
    fine = np.arange(FINE)[:, None] * frequency
    tables = [np.cos(coarse), np.sin(coarse), np.cos(fine), np.sin(fine)]
    return [table.astype(np.float32) for table in tables]


def chunk_count(width):
    for unit in (256, 128):
        if width % unit == 0:
            tiles = width // unit
            return max(n for n in range(1, 8) if tiles % n == 0)
    return 1


def helped_chunks(chunks, places):
    if places < 4:
        return []
    return list(range(1, chunks, 2))


def orders(places):
    table = []
    for p in range(places):
        above, below = list(range(places - 1, p, -1)), list(range(p))
        table.append((above + below if len(above) >= len(below) else below + above) + [p])
    return table


def flipped(index, bit):
    return index + bit - 2 * bit * ((index // bit) % 2)


def kernel(
    dims,
    tokens_ref, wq_ref, wk_ref, wv_ref, pk_ref, pv_ref, wo_ref,
    cc_ref, cs_ref, pre_ref, post_ref, qg_ref, kg_ref, fc_ref, fs_ref,
    out_ref,
    x_buf, wq_buf, wk_buf, wv_buf, q_buf, k_buf, v_buf, wo_buf, wx_buf, att_buf, got_buf, slots, acc_buf, own_buf, we_buf, ea_buf, cc_buf, cs_buf, cos_ref, sin_ref,
    rot_sem, tok_sem, w_sem, prior_sem, wo_sem, own_sem, w_send, w_recv, kv_send, kv_recv, sw_send, sw_recv, s_send, s_recv,
    e_send, e_recv, ea_send, ea_recv,
):
    seq, tp, head, chunks = dims
    rows, width = tokens_ref.shape
    places = tp // 2
    local = rows // tp
    count = 2 * local
    w_rows = wo_ref.shape[0]
    piece = w_rows // seq
    cols = width // chunks
    helped = helped_chunks(chunks, places)
    bits = []
    bit = seq // 2
    while bit >= 1:
        bits.append(bit)
        bit //= 2
    stages = len(bits)
    s = lax.axis_index("seq")
    t = lax.axis_index("tp")
    side = t % 2
    p = t // 2
    mate = t + 1 - 2 * side
    at_end = (p == 0) | (p == places - 1)
    by_end = (p == 1) | (p == places - 2)
    end = jnp.where(p == 1, 0, places - 1)
    scale = float(MODEL_WIDTH // HQ) ** (-0.5)
    f32 = jnp.float32

    parts = 4
    part = rows // parts

    def token_load(i):
        return pltpu.make_async_copy(tokens_ref.at[pl.ds(i * part, part)], x_buf.at[pl.ds(i * part, part)], tok_sem.at[i])

    def wo_load(c):
        return pltpu.make_async_copy(wo_ref.at[:, pl.ds(c * cols, cols)], wo_buf.at[c], wo_sem.at[c])

    weight_loads = [
        pltpu.make_async_copy(src, dst, w_sem.at[i])
        for i, (src, dst) in enumerate(((wk_ref, wk_buf), (wv_ref, wv_buf), (wq_ref, wq_buf)))
    ]
    prior_loads = [
        pltpu.make_async_copy(src, dst.at[pl.ds(0, WINDOW_SPAN)], prior_sem.at[i])
        for i, (src, dst) in enumerate(((pk_ref, k_buf), (pv_ref, v_buf)))
    ]
    own_load = pltpu.make_async_copy(tokens_ref.at[pl.ds(pl.multiple_of(t * local, local), local)], own_buf, own_sem)
    for i in range(parts):
        token_load(i).start()
    weight_loads[0].start()
    coarse_rows = rows // FINE
    table_loads = [
        pltpu.make_async_copy(src.at[pl.ds(pl.multiple_of(s * coarse_rows, 8), coarse_rows)], dst, rot_sem.at[i])
        for i, (src, dst) in enumerate(((cc_ref, cc_buf), (cs_ref, cs_buf)))
    ]
    for load in table_loads:
        load.start()

    @pl.when(s == 0)
    def _():
        for load in prior_loads:
            load.start()

    barrier = pltpu.get_barrier_semaphore()
    near = [(None, (s, mate))]
    near += [(None, (flipped(s, b), t)) for b in bits]
    near += [((s > 0) & (s % 2 == 0), (s - 1, t)), ((s < seq - 1) & (s % 2 == 1), (s + 1, t))]
    near += [(p > 0, (s, t - 2)), (p < places - 1, (s, t + 2))]
    peers = 0
    for there, device in near:
        if there is None:
            peers = peers + 1
            pl.semaphore_signal(barrier, inc=1, device_id=device, device_id_type=MESH)
        else:
            peers = peers + jnp.where(there, 1, 0)

            @pl.when(there)
            def _(device=device):
                pl.semaphore_signal(barrier, inc=1, device_id=device, device_id_type=MESH)
    pl.semaphore_wait(barrier, peers)

    def w_piece(c, index):
        return wx_buf.at[c, pl.ds(pl.multiple_of(index * piece, piece), piece)]

    def w_first(c):
        return pltpu.make_async_remote_copy(
            src_ref=wo_ref.at[pl.ds(pl.multiple_of(s * piece, piece), piece), pl.ds(c * cols, cols)],
            dst_ref=w_piece(c, s),
            send_sem=w_send.at[c, 0],
            recv_sem=w_recv.at[c, 0],
            device_id=(s, mate),
            device_id_type=MESH,
        )

    def masks(stage):
        held = [0]
        for b in bits[: stage - 1]:
            held = held + [m + b for m in held]
        return held

    def from_mask(m):
        index = s
        for b in bits:
            if m & b:
                index = flipped(index, b)
        return index

    def w_next(c, stage, m):
        b = bits[stage - 1]
        index = from_mask(m)
        return pltpu.make_async_remote_copy(
            src_ref=w_piece(c, index),
            dst_ref=w_piece(c, index),
            send_sem=w_send.at[c, m + b],
            recv_sem=w_recv.at[c, m + b],
            device_id=(flipped(s, b), t),
            device_id_type=MESH,
        )

    def w_arrived(c, m):
        pltpu.make_async_remote_copy(
            src_ref=w_piece(c, from_mask(m)),
            dst_ref=w_piece(c, from_mask(m)),
            send_sem=w_send.at[c, m],
            recv_sem=w_recv.at[c, m],
            device_id=(s, mate),
            device_id_type=MESH,
        ).wait_recv()

    def pump(stage, c):
        if stage == 1:
            w_arrived(c, 0)
        else:
            b = bits[stage - 2]
            for m in masks(stage - 1):
                w_arrived(c, m + b)
        for m in masks(stage):
            w_next(c, stage, m).start()

    def w_ready(c):
        if stages == 0:
            w_arrived(c, 0)
        else:
            b = bits[-1]
            for m in masks(stages):
                w_arrived(c, m + b)
        wo_load(c).wait()

    def e_copy(f, half, m, src, index, device):
        return pltpu.make_async_remote_copy(
            src_ref=src,
            dst_ref=we_buf.at[f, half, pl.ds(pl.multiple_of(index * piece, piece), piece)],
            send_sem=e_send.at[f, half, m],
            recv_sem=e_recv.at[f, half, m],
            device_id=device,
            device_id_type=MESH,
        )

    def e_piece(f, half, index):
        return we_buf.at[f, half, pl.ds(pl.multiple_of(index * piece, piece), piece)]

    def e_first(f, m):
        index = from_mask(m)
        src = wo_ref.at[pl.ds(pl.multiple_of(index * piece, piece), piece), pl.ds(helped[f] * cols, cols)]
        return e_copy(f, 0, m, src, index, (s, 2 * jnp.where(p == 0, 1, places - 2) + side))

    def e_mate(f):
        return e_copy(f, 1, 0, e_piece(f, 0, s), s, (s, mate))

    def e_next(f, half, stage, m):
        b = bits[stage - 1]
        index = from_mask(m)
        return e_copy(f, half, m + b, e_piece(f, half, index), index, (flipped(s, b), t))

    def e_arrived(f, half, m):
        index = from_mask(m)
        e_copy(f, half, m, e_piece(f, half, index), index, (s, mate)).wait_recv()

    def e_pump(stage, f):
        @pl.when(by_end)
        def _():
            if stage == 0:
                e_arrived(f, 0, 0)
                e_mate(f).start()
                return
            if stage == 1:
                e_arrived(f, 1, 0)
            else:
                for m in masks(stage - 1):
                    e_arrived(f, 1, m + bits[stage - 2])
            for m in masks(stage):
                e_next(f, 1, stage, m).start()
                if stage == stages:
                    if m:
                        e_arrived(f, 0, m)
                    e_next(f, 0, stage, m).start()

    def e_ready(f):
        @pl.when(by_end)
        def _():
            if stages == 0:
                e_arrived(f, 1, 0)
            else:
                for half in range(2):
                    for m in masks(stages):
                        e_arrived(f, half, m + bits[-1])

    prompt = chunks
    for c in range(prompt):
        w_first(c).start()

    @pl.when(at_end)
    def _():
        for f in range(len(helped)):
            for m in masks(stages):
                e_first(f, m).start()

    for load in table_loads:
        load.wait()
    sign = jnp.where(lax.broadcasted_iota(jnp.int32, (FINE, head), 1) < head // 2, -1.0, 1.0)
    for i in range(coarse_rows):
        far_c, far_s = cc_buf[i : i + 1, :], cs_buf[i : i + 1, :]
        near_c, near_s = fc_ref[...], fs_ref[...]
        cos_ref[i * FINE : (i + 1) * FINE, :] = far_c * near_c - far_s * near_s
        sin_ref[i * FINE : (i + 1) * FINE, :] = (far_s * near_c + far_c * near_s) * sign

    group = 32
    tiles = width // LANES

    for i in range(parts):
        token_load(i).wait()
        if i == parts - 1:
            weight_loads[1].start()
            weight_loads[2].start()

        @pl.loop(0, part // group)
        def _(g, i=i):
            at = pl.ds(pl.multiple_of(i * part + g * group, group), group)
            sums = jnp.zeros((group, LANES), f32)
            for j in range(tiles):
                v = x_buf[at, j * LANES : (j + 1) * LANES].astype(f32)
                sums = sums + v * v
            factor = lax.rsqrt(jnp.sum(sums, axis=-1, keepdims=True) * (1.0 / width) + EPSILON)
            for j in range(tiles):
                v = x_buf[at, j * LANES : (j + 1) * LANES].astype(f32)
                gain = pre_ref[pl.ds(j * LANES, LANES)][None, :]
                x_buf[at, j * LANES : (j + 1) * LANES] = (v * factor * gain).astype(jnp.bfloat16)

    pump(1, 0)

    row_tile = min(512, rows)

    def project(w_buf, first, size, dst, dst_row, gain_ref):
        @pl.loop(0, rows // row_tile)
        def _(i):
            at = pl.ds(pl.multiple_of(i * row_tile, row_tile), row_tile)
            to = pl.ds(pl.multiple_of(dst_row + i * row_tile, row_tile), row_tile)
            raw = jnp.dot(x_buf[at, :], w_buf[:, first : first + size], preferred_element_type=f32)
            if gain_ref is None:
                dst[to, first : first + size] = raw.astype(jnp.bfloat16)
                return
            cosine = cos_ref[at, :]
            sine = sin_ref[at, :]
            for h in range(size // head):
                u = raw[:, h * head : (h + 1) * head]
                mean_square = jnp.mean(u * u, axis=-1, keepdims=True)
                u = u * lax.rsqrt(mean_square + EPSILON) * gain_ref[...][None, :]
                u = u * cosine + pltpu.roll(u, head // 2, 1) * sine
                dst[to, first + h * head : first + (h + 1) * head] = u.astype(jnp.bfloat16)

    def kv_copy(i):
        buf = (k_buf, v_buf)[i]
        return pltpu.make_async_remote_copy(
            src_ref=buf.at[pl.ds(rows, WINDOW_SPAN)],
            dst_ref=buf.at[pl.ds(0, WINDOW_SPAN)],
            send_sem=kv_send.at[i],
            recv_sem=kv_recv.at[i],
            device_id=(s + 1, t),
            device_id_type=MESH,
        )

    q_cols = wq_ref.shape[1]
    kv_cols = wk_ref.shape[1]
    weight_loads[0].wait()
    project(wk_buf, 0, kv_cols, k_buf, WINDOW_SPAN, kg_ref)

    @pl.when(s < seq - 1)
    def _():
        kv_copy(0).start()

    weight_loads[1].wait()
    project(wv_buf, 0, kv_cols, v_buf, WINDOW_SPAN, None)

    @pl.when(s < seq - 1)
    def _():
        kv_copy(1).start()

    weight_loads[2].wait()
    for c in range(chunks):
        wo_load(c).start()
    own_load.start()
    tile = min(256, q_cols)
    for j in range(q_cols // tile):
        project(wq_buf, j * tile, tile, q_buf, 0, qg_ref)
    for c in range(1, min(3, chunks)):
        pump(1, c)
    for stage in range(2, stages + 1):
        pump(stage, 0)

    @pl.when(s == 0)
    def _():
        for load in prior_loads:
            load.wait()

    @pl.when(s > 0)
    def _():
        for i in range(2):
            kv_copy(i).wait_recv()

    table = orders(places)

    def row_block(k):
        r = 0
        for at in range(places):
            for kk in range(places):
                r = r + jnp.where((p == at) & (k == kk), table[at][kk], 0)
        return r

    span = count + WINDOW_SPAN
    group_heads = q_cols // kv_cols

    def attend(k):
        r = row_block(k)
        first = pl.multiple_of(r * count, count)
        row_ids = lax.broadcasted_iota(jnp.int32, (count, count), 0)
        col_ids = lax.broadcasted_iota(jnp.int32, (count, count), 1)
        after = col_ids > row_ids
        for kv in range(kv_cols // head):
            keys = k_buf[pl.ds(first, span), kv * head : (kv + 1) * head]
            values = v_buf[pl.ds(first, span), kv * head : (kv + 1) * head]
            for g in range(group_heads):
                at = slice((kv * group_heads + g) * head, (kv * group_heads + g + 1) * head)
                scores = lax.dot_general(
                    q_buf[pl.ds(first, count), at], keys, (((1,), (1,)), ((), ())), preferred_element_type=f32
                )
                scores = jnp.concatenate(
                    [
                        jnp.where(after, scores[:, :count], -jnp.inf),
                        scores[:, count:WINDOW_SPAN],
                        jnp.where(after, -jnp.inf, scores[:, WINDOW_SPAN:]),
                    ],
                    axis=1,
                )
                highest = jnp.max(scores, axis=-1, keepdims=True)
                weights = jnp.exp2((scores - highest) * (scale * LOG2E))
                total = jnp.sum(weights, axis=-1, keepdims=True)
                mixed = jnp.dot(weights.astype(jnp.bfloat16), values, preferred_element_type=f32)
                mixed = (mixed / total).astype(jnp.bfloat16)
                att_buf[k, 0, :, at] = mixed[:local]
                att_buf[k, 1, :, at] = mixed[local:]

    def swap(k):
        return pltpu.make_async_remote_copy(
            src_ref=att_buf.at[k, 1 - side],
            dst_ref=got_buf.at[k],
            send_sem=sw_send.at[k],
            recv_sem=sw_recv.at[k],
            device_id=(s, mate),
            device_id_type=MESH,
        )

    def product(k, c):
        return jnp.dot(att_buf[k, side], wo_buf[c], preferred_element_type=f32) + jnp.dot(
            got_buf[k], wx_buf[c], preferred_element_type=f32
        )

    def sum_copy(r, slot, c, place):
        return pltpu.make_async_remote_copy(
            src_ref=slots.at[r, c],
            dst_ref=slots.at[slot, c],
            send_sem=s_send.at[r, c],
            recv_sem=s_recv.at[slot, c],
            device_id=(s, 2 * place + side),
            device_id_type=MESH,
        )

    def send_on(r, c):
        @pl.when(r > p)
        def _():
            sum_copy(r, r, c, p + 1).start()

        @pl.when(r < p)
        def _():
            sum_copy(r, jnp.where(r == p - 1, places, r), c, p - 1).start()

    def add_on(k, r, c):
        inner = jnp.where(r > p, p, places - 1 - p) > 0
        total = product(k, c)

        @pl.when(inner)
        def _():
            sum_copy(r, r, c, p).wait_recv()

        total = total + jnp.where(inner, slots[r, c].astype(f32), 0.0)
        slots[r, c] = total.astype(jnp.bfloat16)

    def push(k, c):
        r = row_block(k)
        add_on(k, r, c)
        send_on(r, c)

    def end_product(r, f):
        return jnp.dot(ea_buf[r, 0], we_buf[f, 0], preferred_element_type=f32) + jnp.dot(
            ea_buf[r, 1], we_buf[f, 1], preferred_element_type=f32
        )

    def push_helped(k, c, f):
        r = row_block(k)
        help_here = by_end & (r != end)

        @pl.when(help_here)
        def _():
            if f == 0:
                for half in range(2):
                    end_rows(0, half, r).wait_recv()
            slots[r, c] = (product(k, c) + end_product(r, f)).astype(jnp.bfloat16)

        @pl.when(jnp.logical_not(help_here | at_end))
        def _():
            add_on(k, r, c)

        @pl.when(jnp.logical_not(at_end))
        def _():
            send_on(r, c)

    def end_rows(k, half, r):
        src = got_buf.at[k] if half else att_buf.at[k, side]
        return pltpu.make_async_remote_copy(
            src_ref=src,
            dst_ref=ea_buf.at[r, half],
            send_sem=ea_send.at[k, half],
            recv_sem=ea_recv.at[r, half],
            device_id=(s, 2 * jnp.where(p == 0, 1, places - 2) + side),
            device_id_type=MESH,
        )

    @pl.loop(0, places)
    def _(k):
        attend(k)
        swap(k).start()

        @pl.when(k == 0)
        def _():
            w_ready(0)

        for c in range(prompt, min(chunks, prompt + places)):
            @pl.when(k == c - prompt)
            def _(c=c):
                w_first(c).start()

        if chunks > 3:
            @pl.when(k == 0)
            def _():
                pump(1, 3)

        for f in range(min(len(helped), places)):
            @pl.when(k == f)
            def _(f=f):
                e_pump(0, f)

        for f in range(min(len(helped), places - 2)):
            @pl.when(k == f + 2)
            def _(f=f):
                e_pump(1, f)

        @pl.when(k >= 1)
        def _():
            swap(k - 1).wait_recv()
            push(k - 1, 0)

            if helped:
                @pl.when(at_end & (k == places - 2))
                def _():
                    for kk in range(places - 2):
                        for half in range(2):
                            end_rows(kk, half, row_block(kk)).start()

    for c in range(prompt + places, chunks):
        w_first(c).start()
    for f in range(places, len(helped)):
        e_pump(0, f)
    waiting = []
    for c in range(3, chunks):
        if c >= 4:
            waiting.append((c, False))
        if c in helped and helped.index(c) >= places - 2:
            waiting.append((c, True))
    for c in range(1, chunks):
        taken = 0
        while waiting and (taken < 2 or waiting[0][0] <= c):
            which, ends = waiting.pop(0)
            if stages == 0:
                continue
            if ends:
                e_pump(1, helped.index(which))
            else:
                pump(1, which)
            taken += 1
        for stage in range(2, stages + 1):
            pump(stage, c)
            if c in helped:
                e_pump(stage, helped.index(c))
        w_ready(c)
        if c not in helped:
            @pl.loop(0, places - 1)
            def _(k, c=c):
                push(k, c)
        else:
            f = helped.index(c)
            e_ready(f)
            @pl.loop(0, places - 1)
            def _(k, c=c, f=f):
                push_helped(k, c, f)
    if helped:
        @pl.when(at_end)
        def _():
            for half in range(2):
                end_rows(places - 2, half, row_block(places - 2)).start()

    last = places - 1
    swap(last).wait_recv()
    own_load.wait()

    def finish(c, square):
        total = product(last, c)
        ahead, behind = p > 0, p < places - 1
        if c in helped:
            ahead, behind = ahead & (p != 1), behind & (p != places - 2)
            acc_buf[c] = total

            @pl.when(by_end)
            def _():
                if c == helped[0]:
                    for half in range(2):
                        end_rows(0, half, p).wait_recv()
                acc_buf[c] += end_product(p, helped.index(c))

            total = acc_buf[c]

        @pl.when(ahead)
        def _():
            sum_copy(p, p, c, p).wait_recv()

        @pl.when(behind)
        def _():
            sum_copy(p, places, c, p).wait_recv()

        total = total + jnp.where(ahead, slots[p, c].astype(f32), 0.0)
        total = total + jnp.where(behind, slots[places, c].astype(f32), 0.0)
        acc_buf[c] = total
        return square + jnp.sum(total * total, axis=-1, keepdims=True)

    square = jnp.zeros((local, 1), f32)
    for c in range(chunks):
        square = finish(c, square)
    factor = lax.rsqrt(square * (1.0 / width) + EPSILON)
    for c in range(chunks):
        at = slice(c * cols, (c + 1) * cols)
        out_ref[:, at] = (own_buf[:, at].astype(f32) + acc_buf[c] * factor * post_ref[pl.ds(c * cols, cols)][None, :]).astype(out_ref.dtype)

    for c in range(chunks):
        w_first(c).wait_send()
    if stages:
        @pl.loop(0, chunks)
        def _(c):
            for stage in range(1, stages + 1):
                for m in masks(stage):
                    w_next(c, stage, m).wait_send()

    @pl.when(s < seq - 1)
    def _():
        for i in range(2):
            kv_copy(i).wait_send()

    @pl.loop(0, places)
    def _(k):
        swap(k).wait_send()

        @pl.when(k < places - 1)
        def _():
            r = row_block(k)

            for c in range(chunks):
                if c in helped:
                    @pl.when(jnp.logical_not(at_end))
                    def _(c=c):
                        sum_copy(r, r, c, p).wait_send()
                else:
                    sum_copy(r, r, c, p).wait_send()

    if helped:
        @pl.when(at_end)
        def _():
            for f in range(len(helped)):
                for m in masks(stages):
                    e_first(f, m).wait_send()

            @pl.loop(0, places - 1)
            def _(k):
                for half in range(2):
                    end_rows(k, half, row_block(k)).wait_send()

        @pl.when(by_end)
        def _():
            for f in range(len(helped)):
                e_mate(f).wait_send()
                for stage in range(1, stages + 1):
                    for m in masks(stage):
                        e_next(f, 1, stage, m).wait_send()
                        if stage == stages:
                            e_next(f, 0, stage, m).wait_send()


def sublayer(
    sizes,
    tokens,
    pre_gain,
    w_query,
    key_weight_matrix,
    value_weight_matrix,
    query_gain,
    key_norm_gain,
    prior_key_cache,
    prior_value_cache,
    w_out,
    post_gain,
):
    seq, tp = sizes
    rows, width = tokens.shape
    head = query_gain.shape[0]
    q_cols, kv_cols = w_query.shape[1], key_weight_matrix.shape[1]
    w_rows = w_out.shape[0]
    local = rows // tp
    places = tp // 2
    chunks = chunk_count(width)
    cols = width // chunks
    helped = len(helped_chunks(chunks, places))
    tables = rotary_tables(head // 2, WINDOW_SPAN, seq * rows)
    bf16, f32 = jnp.bfloat16, jnp.float32
    dma = pltpu.SemaphoreType.DMA
    anywhere = pl.BlockSpec(memory_space=pl.ANY)
    vmem = pl.BlockSpec(memory_space=pltpu.VMEM)
    return pl.pallas_call(
        functools.partial(kernel, (seq, tp, head, chunks)),
        out_shape=jax.ShapeDtypeStruct((local, width), tokens.dtype),
        in_specs=[anywhere] * 9 + [vmem] * 6,
        out_specs=vmem,
        scratch_shapes=[
            pltpu.VMEM((rows, width), bf16),
            pltpu.VMEM((width, q_cols), bf16),
            pltpu.VMEM((width, kv_cols), bf16),
            pltpu.VMEM((width, kv_cols), bf16),
            pltpu.VMEM((rows, q_cols), bf16),
            pltpu.VMEM((WINDOW_SPAN + rows, kv_cols), bf16),
            pltpu.VMEM((WINDOW_SPAN + rows, kv_cols), bf16),
            pltpu.VMEM((chunks, w_rows, cols), bf16),
            pltpu.VMEM((chunks, w_rows, cols), bf16),
            pltpu.VMEM((places, 2, local, q_cols), bf16),
            pltpu.VMEM((places, local, q_cols), bf16),
            pltpu.VMEM((places + 1, chunks, local, cols), bf16),
            pltpu.VMEM((chunks, local, cols), f32),
            pltpu.VMEM((local, width), bf16),
            pltpu.VMEM((max(helped, 1), 2, w_rows, cols), bf16),
            pltpu.VMEM((places, 2, local, q_cols), bf16),
            pltpu.VMEM((rows // FINE, head), f32),
            pltpu.VMEM((rows // FINE, head), f32),
            pltpu.VMEM((rows, head), f32),
            pltpu.VMEM((rows, head), f32),
            dma((2,)),
            dma((4,)),
            dma((3,)),
            dma((2,)),
            dma((chunks,)),
            dma,
            dma((chunks, seq)),
            dma((chunks, seq)),
            dma((2,)),
            dma((2,)),
            dma((places,)),
            dma((places,)),
            dma((places + 1, chunks)),
            dma((places + 1, chunks)),
            dma((max(helped, 1), 2, seq)),
            dma((max(helped, 1), 2, seq)),
            dma((places, 2)),
            dma((places, 2)),
        ],
        compiler_params=pltpu.CompilerParams(
            collective_id=0, has_side_effects=True, vmem_limit_bytes=63 * 1024 * 1024
        ),
        cost_estimate=pl.CostEstimate(
            flops=2 * rows * width * (q_cols + 2 * kv_cols + 2 * w_rows),
            bytes_accessed=2 * (rows * width + width * (q_cols + 2 * kv_cols) + w_rows * width),
            transcendentals=0,
        ),
    )(
        tokens,
        w_query,
        key_weight_matrix,
        value_weight_matrix,
        prior_key_cache,
        prior_value_cache,
        w_out,
        tables[0],
        tables[1],
        pre_gain,
        post_gain,
        query_gain,
        key_norm_gain,
        tables[2],
        tables[3],
    )


def solution(mesh):
    sizes = (mesh.shape["seq"], mesh.shape["tp"])
    return jax.shard_map(
        functools.partial(sublayer, sizes),
        mesh=mesh,
        in_specs=(
            P("seq", None),
            P(),
            P(None, "tp"),
            P(None, "tp"),
            P(None, "tp"),
            P(),
            P(),
            P(None, "tp"),
            P(None, "tp"),
            P("tp", None),
            P(),
        ),
        out_specs=P(("seq", "tp"), None),
        check_vma=False,
    )
```
